32 devices in a mesh: site: 2 (over y), handler: 4 (over x, core), worker: 4 (over z).
Axes of the slice: x: 2, y: 2, z: 4, core: 2. Of those that a mesh axis runs over, the one named last changes fastest.
Arguments:
- sgt: bfloat16 [2048, 6, 3, 1024], P(('site', 'handler', 'worker')), parts along dimension 0, may hold values from -6 to 6
- mechanism: bfloat16 [6, 1024], P(None, ('handler', 'worker')), may hold values from -2.5 to 2.5
- req_owner: int32 [1024, 1], P(('site', 'handler', 'worker')), parts along dimension 0, may hold values from 0 to 15; in each aligned block of 32 rows (0 to 31, 32 to 63, ...) at most 4 rows name the same one
- req_local: int32 [1024], P(('site', 'handler', 'worker')), parts along dimension 0, may hold values from 0 to 31
- slip: bfloat16 [1024, 64, 128], P(('site', 'handler', 'worker')), parts along dimension 0, may hold values from 0 to 0.029907227
Outputs:
- seismograms: float32 [32, 64, 3, 1024], P(('site', 'handler'), 'worker'), parts along dimension 0
The draws below stay inside these ranges and needn't reach their ends.
There are 2 independent parts, one for each index of `site`. The reference program is written for one: setup_inputs(seed, part) draws one part's arguments, and reference() takes and returns one part's arrays. A program takes and returns all parts, laid end to end along the dimension named above; an argument that names none is the same for every part. Nothing has to cross between parts.
Inputs may be any that keep to these rules, and one draw needn't show every extreme that they name: `req_owner`: among the 32 requests of one device no owner is named more than 4 times, and in every draw some device names some owner exactly 4 times; every owner is named somewhere.
All inputs are finite; a program needn't handle non-finite values.
Results may differ from the reference program's by a relative error of at most 0.0029.
Values may be sent and summed in bfloat16 or wider, within the bound.
No kernel may reach another device: no remote copies, remote signals or barrier semaphores. Data moves between devices by JAX's collectives and lax.ppermute only.
A program may use at most 128 MiB of HBM per device.

```python
import math
import jax
import jax.numpy as jnp
import numpy as np
from jax import lax

SAMPLES = 1024
VARS = 64
TAPS = 64
BLK = 2
RUP_SLOTS = 4
REQ = 32
PTS_DEV = 64
POINTS = 1024
REQUESTS = 512
RUPTURES = 16
CAP = 4
N_HANDLER = 4
N_WORKER = 4


def with_ends(drawn, key, smallest, largest):
    shape = drawn.shape
    spot = [jax.random.randint(jax.random.fold_in(key, axis), (), 0, shape[axis]) for axis in range(len(shape))]
    drawn = drawn.at[tuple(spot)].set(smallest)
    longest = shape.index(max(shape))
    spot[longest] = (spot[longest] + 1) % shape[longest]
    return drawn.at[tuple(spot)].set(largest)


def block_levels(key, dims, split, least, top_value):
    def one(axis_at, parts):
        heights = jax.random.uniform(jax.random.fold_in(jax.random.fold_in(key, 6), axis_at), (parts,), jnp.float32, least / len(split), top_value / len(split))
        return jnp.repeat(jnp.exp(heights), dims[axis_at] // parts).reshape((-1,) + (1,) * (len(dims) - axis_at - 1))

    loudness = one(*split[0])
    for cut in split[1:]:
        loudness = loudness * one(*cut)
    return loudness


def deal_out(key, own, number, rows, amount, top, limit, slope):
    sequence = jax.random.permutation(key, amount)
    packed, usual = portions_of(amount, rows * top, limit, slope, True), portions_of(amount, rows * top, limit, slope, False)
    places = jnp.arange(amount)

    def named(lengths, turn):
        used = int((lengths > 0).sum())
        fixed = max(1, used // 4)
        shifted = fixed + (places - fixed + turn * (used - fixed)) % max(1, amount - fixed)
        return jnp.zeros((amount,), jnp.int32).at[sequence[jnp.where(places < fixed, places, shifted)]].set(jnp.asarray(lengths, jnp.int32))

    lengths = jnp.where(number % 4 == 0, named(packed, number // 4), named(usual, number - number // 4 - 1))
    mixed = jax.random.permutation(jax.random.fold_in(own, 3), amount)
    donor, sink = mixed[0:amount // 2 * 2:2], mixed[1:amount // 2 * 2:2]
    margin = jnp.minimum(lengths[donor] - 1, limit - lengths[sink]) // 2
    margin = jnp.where((donor == sequence[0]) | (sink == sequence[0]) | (lengths[sink] == 0), 0, jnp.maximum(margin, 0))
    shifted = jax.random.randint(jax.random.fold_in(own, 4), (amount // 2,), 0, 1 << 20) % (margin + 1)
    lengths = lengths.at[donor].add(-shifted).at[sink].add(shifted)
    members = jnp.searchsorted(jnp.cumsum(lengths), jnp.arange(rows * top), side="right").astype(jnp.int32)
    table = members.reshape(top, rows).T
    table = table[jax.random.permutation(jax.random.fold_in(own, 1), rows)]
    turn = jax.random.randint(jax.random.fold_in(own, 2), (rows, 1), 0, top)
    return jnp.take_along_axis(table, (jnp.arange(top)[None, :] + turn) % top, axis=1)


def portions_of(amount, total, reach, lean, full):
    loads = [(1 << 20) // math.isqrt(standing ** lean) + 1 for standing in range(1, amount + 1)]
    largest = reach if full else min(reach, max(-(-total // amount), total * loads[0] // sum(loads)))
    least = 1 if total - largest >= amount - 1 else 0
    given, spare = [largest] + [least] * (amount - 1), total - largest - least * (amount - 1)
    while spare > 0:
        free = [i for i in range(1, amount) if given[i] < largest] or [i for i in range(1, amount) if given[i] < reach]
        pool, left = sum([loads[i] for i in free]), spare
        for i in free:
            more = min(reach - given[i], max(1, left * loads[i] // pool), spare)
            given[i] = given[i] + more
            spare = spare - more
    return np.array(given)


def gaussian(key, dims, spread, most, split=(), dtype=jnp.bfloat16):
    drawn = spread * jax.random.normal(key, dims, jnp.float32)
    if split:
        drawn = drawn * block_levels(key, dims, split, -0.22, 0.18)
    return jnp.clip(drawn, -most, most).astype(dtype)


def setup_inputs(seed: int = 0, part: int = 0) -> dict:
    seeds = jax.random.split(jax.random.key(seed), 6)
    own_keys = jax.random.split(jax.random.fold_in(seeds[5], part), 6)
    sgt = gaussian(own_keys[0], (POINTS, 6, 3, SAMPLES), 1.0, 6.0, ((0, 16),))
    mechanism = gaussian(seeds[1], (6, POINTS), 6 ** -0.5, 2.5, ((1, 16),))
    req_owner_keys = jax.random.split(jax.random.fold_in(own_keys[2], 1), REQUESTS // REQ)
    req_owner_turns = jax.random.permutation(jax.random.fold_in(own_keys[2], 3), REQUESTS // REQ)
    req_owner = jax.vmap(lambda own, number: deal_out(jax.random.fold_in(own_keys[2], 2), own, number, REQ, N_HANDLER * N_WORKER, 1, CAP, 2))(req_owner_keys, req_owner_turns).reshape((REQUESTS, 1))
    req_local = with_ends(jax.random.randint(own_keys[3], (REQUESTS,), 0, PTS_DEV // BLK), jax.random.fold_in(own_keys[3], 1), 0, (PTS_DEV // BLK) - 1).astype(jnp.int32)
    slip = jnp.clip(0.029907227 * jax.random.uniform(own_keys[4], (REQUESTS, VARS, BLK * TAPS), jnp.float32) ** block_levels(own_keys[4], (REQUESTS, VARS, BLK * TAPS), ((0, 16),), -0.2, 0.2), 0.0, 0.029907227).astype(jnp.bfloat16)
    return dict(sgt=sgt, mechanism=mechanism, req_owner=req_owner, req_local=req_local, slip=slip)


def combine_points(sgt, mechanism):
    total = mechanism[0].astype(jnp.float32)[:, None, None] * sgt[:, 0].astype(jnp.float32)
    for comp in range(1, 6):
        total = total + mechanism[comp].astype(jnp.float32)[:, None, None] * sgt[:, comp].astype(jnp.float32)
    return total.astype(jnp.bfloat16)


def shifted_blocks(green):
    samples = green.shape[-1]
    padded = jnp.pad(green, ((0, 0), (0, 0), (0, 0), (TAPS, 0)))
    return jnp.stack([padded[..., TAPS - lag:TAPS - lag + samples] for lag in range(TAPS)], axis=2)


def device_partial(blocks, slip_rows):
    rows = blocks.shape[0] // RUP_SLOTS
    samples = blocks.shape[-1]
    outputs = []
    for slot in range(RUP_SLOTS):
        stacked = shifted_blocks(blocks[slot * rows:(slot + 1) * rows])
        right = stacked.reshape(rows * BLK * TAPS, 3 * samples)
        left = jnp.transpose(slip_rows[slot * rows:(slot + 1) * rows], (1, 0, 2)).reshape(VARS, rows * BLK * TAPS)
        outputs.append(jnp.dot(left, right, preferred_element_type=jnp.float32).reshape(VARS, 3, samples))
    return jnp.stack(outputs, axis=0)


def reference(sgt, mechanism, req_owner, req_local, slip):
    devices_part = N_HANDLER * N_WORKER
    per_owner = PTS_DEV // BLK
    green = combine_points(sgt, mechanism)
    green_blocks = green.reshape(POINTS // BLK, BLK, 3, SAMPLES)
    block_ids = (req_owner[:, 0] * per_owner + req_local).astype(jnp.int32)
    block_ids = block_ids.reshape(devices_part, REQ)
    slip_dev = slip.reshape(devices_part, REQ, VARS, BLK * TAPS)

    def one_device(pair):
        ids, slip_rows = pair
        return device_partial(green_blocks[ids], slip_rows)

    partial_value = lax.map(one_device, (block_ids, slip_dev))
    partial_value = partial_value.reshape(N_HANDLER, N_WORKER, RUP_SLOTS, VARS, 3, SAMPLES)
    return jnp.sum(partial_value, axis=1).reshape(RUPTURES, VARS, 3, SAMPLES)
```

```python
import functools

import jax
import jax.numpy as jnp
from jax import lax
from jax.experimental import pallas as pl
from jax.experimental.pallas import tpu as pltpu
from jax.sharding import PartitionSpec as P

TAPS = 64
BLK = 2
RUP_SLOTS = 4
LANES = 128
SUB = 8
VMEM_BUDGET = 12 * 1024 * 1024
MIB = 1024 * 1024
BF = jnp.bfloat16
F32 = jnp.float32


def combine_points(sgt, mechanism):
    total = mechanism[0].astype(jnp.float32)[:, None, None] * sgt[:, 0].astype(jnp.float32)
    for comp in range(1, 6):
        total = total + mechanism[comp].astype(jnp.float32)[:, None, None] * sgt[:, comp].astype(
            jnp.float32
        )
    return total.astype(jnp.bfloat16)


def shifted_blocks(green):
    samples = green.shape[-1]
    padded = jnp.pad(green, ((0, 0), (0, 0), (0, 0), (TAPS, 0)))
    return jnp.stack(
        [padded[..., TAPS - lag : TAPS - lag + samples] for lag in range(TAPS)], axis=2
    )


def deliver(first, second):
    return (
        lax.all_to_all(first, ("handler", "worker"), split_axis=0, concat_axis=0, tiled=True),
        lax.all_to_all(second, ("handler", "worker"), split_axis=0, concat_axis=0, tiled=True),
    )


def local_exchange(sgt, mechanism, req_owner, req_local, slip):
    peers = lax.axis_size(("handler", "worker"))
    samples = sgt.shape[-1]
    blocks_here = sgt.shape[0] // BLK
    requests = req_local.shape[0]
    capacity = max(2, (2 * requests + peers - 1) // peers)
    owner = req_owner[:, 0]
    member = (owner[:, None] == jnp.arange(peers, dtype=jnp.int32)[None, :]).astype(jnp.int32)
    earlier = jnp.sum((jnp.cumsum(member, axis=0) - member) * member, axis=1)
    position = owner * capacity + earlier
    table = jnp.full((peers * capacity,), -1, jnp.int32).at[position].set(req_local)
    asked = lax.all_to_all(
        table.reshape(peers, capacity),
        ("handler", "worker"),
        split_axis=0,
        concat_axis=0,
        tiled=True,
    )
    wanted = (asked >= 0).reshape(-1)
    picked = jnp.where(wanted, asked.reshape(-1), 0)
    green_here = combine_points(sgt, mechanism).reshape(blocks_here, BLK, 3, samples)
    chosen = jnp.where(wanted[:, None, None, None], green_here[picked], jnp.zeros((), jnp.bfloat16))
    chosen = chosen.reshape(peers, capacity, BLK, 3, samples)
    front, back = deliver(chosen[:, :, :, :2], chosen[:, :, :, 2:])
    arrived = jnp.concatenate([front, back], axis=3)
    blocks = arrived.reshape(peers * capacity, BLK, 3, samples)[position]
    rows = requests // RUP_SLOTS
    variations = slip.shape[1]
    outputs = []
    for slot in range(RUP_SLOTS):
        stacked = shifted_blocks(blocks[slot * rows : (slot + 1) * rows])
        right = stacked.reshape(rows * BLK * TAPS, 3 * samples)
        left = jnp.transpose(slip[slot * rows : (slot + 1) * rows], (1, 0, 2)).reshape(
            variations, rows * BLK * TAPS
        )
        outputs.append(
            jnp.dot(left, right, preferred_element_type=jnp.float32).reshape(variations, 3, samples)
        )
    partial_value = jnp.stack(outputs, axis=0)
    return lax.psum_scatter(partial_value, "worker", scatter_dimension=1, tiled=True)


def combine_kernel(samples, sgt_ref, mech_ref, same_ref, other_ref, mech_scratch):
    step = pl.program_id(0)
    count = same_ref.shape[0]

    @pl.when(step == 0)
    def _():
        mech_scratch[...] = jnp.transpose(mech_ref[...].astype(F32))

    mech = mech_scratch[pl.ds(pl.multiple_of(step * count, count), count), :]
    green = []
    for k in range(3):
        total = mech[:, 0:1] * sgt_ref[0, k].astype(F32)
        for comp in range(1, 6):
            total = total + mech[:, comp : comp + 1] * sgt_ref[comp, k].astype(F32)
        green.append(total.astype(BF))
    half = samples // 2
    parity = lax.rem(lax.axis_index("worker"), 2)

    def write(low_ref, high_ref):
        low_ref[:, :samples] = green[0]
        low_ref[:, samples : samples + LANES] = jnp.zeros((count, LANES), BF)
        low_ref[:, samples + LANES :] = green[1][:, :half]
        high_ref[:, :samples] = green[2]
        high_ref[:, samples:] = green[1][:, half - LANES :]

    @pl.when(parity == 0)
    def _():
        write(same_ref, other_ref)

    @pl.when(parity == 1)
    def _():
        write(other_ref, same_ref)


def combine(sgt, mechanism):
    points, comps, kinds, samples = sgt.shape
    width = samples + LANES + samples // 2
    step = min(16, points)
    out = jax.ShapeDtypeStruct((points, width), BF)
    return pl.pallas_call(
        functools.partial(combine_kernel, samples),
        grid=(points // step,),
        in_specs=[
            pl.BlockSpec((comps, kinds, step, samples), lambda p: (0, 0, p, 0)),
            pl.BlockSpec((comps, points), lambda p: (0, 0)),
        ],
        out_specs=[pl.BlockSpec((step, width), lambda p: (p, 0))] * 2,
        out_shape=[out, out],
        scratch_shapes=[pltpu.VMEM((points, comps), F32)],
        compiler_params=pltpu.CompilerParams(vmem_limit_bytes=16 * MIB),
        name="combine",
    )(jnp.transpose(sgt, (1, 2, 0, 3)), mechanism)


def group_transpose(rows, lane):
    rows = list(rows)
    count = len(rows)
    step = count // 2
    while step:
        keep = (lane // (SUB * step)) % 2 == 0
        for j in range(count):
            if j & step:
                continue
            low, high = rows[j], rows[j + step]
            rows[j] = jnp.where(keep, low, pltpu.roll(high, SUB * step, 1))
            rows[j + step] = jnp.where(keep, pltpu.roll(low, LANES - SUB * step, 1), high)
        step //= 2
    return rows


def turn_kernel(workers, slip_ref, own_ref, *rest):
    others, grouped = rest[:-1], rest[-1]
    outs = (own_ref, *others)
    slots, coarse, group, _ = own_ref.shape
    rows = slip_ref.shape[0] // slots
    mine = lax.axis_index("worker") // 2
    tall = 2 * SUB
    lane = lax.broadcasted_iota(jnp.int32, (tall, LANES), 1)
    source = lax.broadcasted_iota(jnp.int32, (LANES, LANES), 0)
    target = lax.broadcasted_iota(jnp.int32, (LANES, LANES), 1)
    fine, row, point = source % SUB, (source % TAPS) // SUB, source // TAPS
    place = jnp.where(target == (fine * rows + row) * BLK + point, 1.0, 0.0).astype(BF)

    def body(slot, carry):
        for g, out in enumerate(outs):
            for v in range(0, group, tall):
                at = pl.multiple_of((mine ^ g) * group + v, tall)
                turned = group_transpose(
                    [slip_ref[slot * rows + n, pl.ds(at, tall), :] for n in range(rows)], lane
                )
                for a in range(coarse):
                    grouped[a * group + v : a * group + v + tall, :] = turned[a]
            moved = jnp.dot(grouped[...], place, preferred_element_type=F32).astype(BF)
            for a in range(coarse):
                out[slot, a] = moved[a * group : (a + 1) * group]
        return carry

    lax.fori_loop(0, slots, body, 0)


def turn_slip(slip, workers):
    requests, variations, depth = slip.shape
    groups = workers // 2
    group = variations // groups
    out = jax.ShapeDtypeStruct((RUP_SLOTS, TAPS // SUB, group, depth), BF)
    vmem = pl.BlockSpec(memory_space=pltpu.VMEM)
    return pl.pallas_call(
        functools.partial(turn_kernel, workers),
        in_specs=[vmem],
        out_specs=[vmem] * groups,
        out_shape=[out] * groups,
        scratch_shapes=[pltpu.VMEM((TAPS // SUB * group, depth), BF)],
        compiler_params=pltpu.CompilerParams(vmem_limit_bytes=8 * MIB),
        name="turn_slip",
    )(slip)


def convolve_kernel(pieces, sources, *refs):
    rows_ref = refs[0]
    green = refs[1 : 1 + pieces]
    slips = refs[1 + pieces : 1 + pieces + sources]
    own_ref, send_ref, hot, dense, left, right, product = refs[1 + pieces + sources :]
    points, width = green[0].shape
    slots, coarse, group, _ = slips[0].shape
    per_source = rows_ref.shape[0] // (slots * sources)
    tiles = width // LANES
    samples = (width - LANES) * 2 // 3
    first = samples // LANES
    parity = lax.rem(lax.axis_index("worker"), 2)
    span = 2 * LANES

    asked = rows_ref[...]
    for c in range(0, pieces * points, LANES):
        column = lax.broadcasted_iota(jnp.int32, (asked.shape[0], LANES), 1) + c
        hot[:, c : c + LANES] = jnp.where(asked == column, 1.0, 0.0).astype(BF)
    together = max(1, span // points)
    for c in range(0, width, span):
        e = min(width, c + span)
        total = None
        for p in range(0, pieces, together):
            block = jnp.concatenate([g[:, c:e] for g in green[p : p + together]], axis=0)
            part = jnp.dot(
                hot[:, p * points : (p + together) * points], block, preferred_element_type=F32
            )
            total = part if total is None else total + part
        dense[:, c:e] = total.astype(BF)

    lane = lax.broadcasted_iota(jnp.int32, (SUB, LANES), 1)
    wide_lane = lax.broadcasted_iota(jnp.int32, (per_source, LANES), 1)
    zero = jnp.zeros((SUB, LANES), F32)

    def slot_body(slot, carry):
        for j in range(sources):
            for a in range(coarse):
                left[a * group : (a + 1) * group, j * LANES : (j + 1) * LANES] = slips[j][slot, a]
            at = pl.multiple_of((slot * sources + j) * per_source, per_source)
            for b in range(SUB):
                put = j * LANES + b * per_source
                before = jnp.zeros((per_source, LANES), BF)
                for m in range(tiles):
                    value = dense[pl.ds(at, per_source), m * LANES : (m + 1) * LANES]
                    if b:
                        turn = pltpu.roll(value, b, 1)
                        if m == first:
                            before = jnp.zeros((per_source, LANES), BF)
                        value = jnp.where(wide_lane < b, before, turn)
                        before = turn
                    right[put : put + per_source, m * LANES : (m + 1) * LANES] = value

        for c in range(0, width, span):
            e = min(width, c + span)
            product[:, c:e] = jnp.dot(left[...], right[:, c:e], preferred_element_type=F32)

        for side in range(2):
            for u in range(0, group // 2, SUB):
                total = [None] * tiles
                for a in range(coarse):
                    start = pl.multiple_of(
                        a * group + lax.rem(parity + side, 2) * (group // 2) + u, SUB
                    )
                    before = zero
                    for m in range(tiles):
                        value = product[pl.ds(start, SUB), m * LANES : (m + 1) * LANES]
                        if a:
                            value = pltpu.roll(value, a * SUB, 1)
                        if m == first:
                            before = zero
                        moved = jnp.where(lane < a * SUB, before, value) if a else value
                        before = value
                        total[m] = moved if total[m] is None else total[m] + moved
                total = total[:first] + total[first + 1 :]
                for m, value in enumerate(total):
                    if side == 0:
                        own_ref[slot, u : u + SUB, m * LANES : (m + 1) * LANES] = value
                    else:
                        send_ref[slot, u : u + SUB, m * LANES : (m + 1) * LANES] = value.astype(BF)
        return carry

    lax.fori_loop(0, slots, slot_body, 0)


def convolve(rows, green, slips):
    points, width = green[0].shape
    slots, coarse, group, depth = slips[0].shape
    inner = depth * len(slips)
    vmem = pl.BlockSpec(memory_space=pltpu.VMEM)
    return pl.pallas_call(
        functools.partial(convolve_kernel, len(green), len(slips)),
        in_specs=[vmem] * (1 + len(green) + len(slips)),
        out_specs=[vmem, vmem],
        out_shape=[
            jax.ShapeDtypeStruct((slots, group // 2, width - LANES), F32),
            jax.ShapeDtypeStruct((slots, group // 2, width - LANES), BF),
        ],
        scratch_shapes=[
            pltpu.VMEM((rows.shape[0], len(green) * points), BF),
            pltpu.VMEM((rows.shape[0], width), BF),
            pltpu.VMEM((coarse * group, inner), BF),
            pltpu.VMEM((inner, width), BF),
            pltpu.VMEM((coarse * group, width), F32),
        ],
        compiler_params=pltpu.CompilerParams(vmem_limit_bytes=16 * MIB),
        name="convolve",
    )(rows, *green, *slips)


def assemble_kernel(own_ref, got_ref, out_ref):
    slots, kinds, group, samples = out_ref.shape
    half = samples // 2
    parity = lax.rem(lax.axis_index("worker"), 2)

    def write(low, high):
        out_ref[0, 0] = low[0, :, :samples].astype(F32)
        out_ref[0, 1, :, :half] = low[0, :, samples:].astype(F32)
        out_ref[0, 1, :, half:] = high[0, :, samples:].astype(F32)
        out_ref[0, 2] = high[0, :, :samples].astype(F32)

    @pl.when(parity == 0)
    def _():
        write(own_ref, got_ref)

    @pl.when(parity == 1)
    def _():
        write(got_ref, own_ref)


def assemble(own, got, samples):
    slots, group, width = own.shape
    spec = pl.BlockSpec((1, group, width), lambda r: (r, 0, 0))
    return pl.pallas_call(
        assemble_kernel,
        grid=(slots,),
        in_specs=[spec, spec],
        out_specs=pl.BlockSpec((1, 3, group, samples), lambda r: (r, 0, 0, 0)),
        out_shape=jax.ShapeDtypeStruct((slots, 3, group, samples), F32),
        compiler_params=pltpu.CompilerParams(vmem_limit_bytes=8 * MIB),
        name="assemble",
    )(own, got)


def swap(value, axis, flip):
    return lax.ppermute(value, axis, [(i, i ^ flip) for i in range(lax.axis_size(axis))])


def local_replicate(sgt, mechanism, req_owner, req_local, slip):
    handlers, workers = lax.axis_size("handler"), lax.axis_size("worker")
    handler, worker = lax.axis_index("handler"), lax.axis_index("worker")
    points, _, _, samples = sgt.shape
    blocks_here = points // BLK
    requests = req_local.shape[0]
    same, other = combine(sgt, mechanism)

    green = {(0, 0): same}
    for flip in [*range(2, workers), 1]:
        green[0, flip] = swap(other if flip % 2 else same, "worker", flip)
    bit = handlers // 2
    while bit:
        for (hand, flip), value in list(green.items()):
            green[hand ^ bit, flip] = swap(value, "handler", bit)
        bit //= 2

    turned = turn_slip(slip, workers)
    slips = {0: turned[0], 1: swap(turned[0], "worker", 1)}
    for flip in range(2, workers, 2):
        slips[flip] = swap(turned[flip // 2], "worker", flip)
        slips[flip + 1] = swap(slips[flip], "worker", 1)

    code = req_owner[:, 0] * blocks_here + req_local
    codes = jnp.stack([code] + [swap(code, "worker", flip) for flip in range(1, workers)])
    owner = codes // blocks_here
    piece = ((owner // workers) ^ handler) * workers + ((owner % workers) ^ worker)
    row = piece * points + codes % blocks_here * BLK
    row = jnp.transpose(row.reshape(workers, RUP_SLOTS, requests // RUP_SLOTS), (1, 0, 2))
    rows = (row[..., None] + jnp.arange(BLK, dtype=jnp.int32)).reshape(-1, 1)
    own, send = convolve(
        rows,
        [green[hand, flip] for hand in range(handlers) for flip in range(workers)],
        [slips[flip] for flip in range(workers)],
    )
    got = swap(send, "worker", 1)
    return jnp.transpose(assemble(own, got, samples), (0, 2, 1, 3))


def power_of_two(count):
    return count & (count - 1) == 0


def local(sgt, mechanism, req_owner, req_local, slip):
    handlers, workers = lax.axis_size("handler"), lax.axis_size("worker")
    points, comps, kinds, samples = sgt.shape
    width = samples + samples // 2 + LANES
    fits = handlers * workers * points * width * 4 <= VMEM_BUDGET
    shaped = (
        power_of_two(handlers)
        and power_of_two(workers)
        and workers >= 2
        and kinds == 3
        and samples % (2 * LANES) == 0
        and slip.shape[2] == BLK * TAPS == LANES
        and req_local.shape[0] // RUP_SLOTS == TAPS // SUB
        and slip.shape[1] % (workers * SUB) == 0
    )
    plan = local_replicate if fits and shaped else local_exchange
    return plan(sgt, mechanism, req_owner, req_local, slip)


def solution(mesh):
    return jax.shard_map(
        local,
        mesh=mesh,
        in_specs=(
            P(("site", "handler", "worker"), None, None, None),
            P(None, ("handler", "worker")),
            P(("site", "handler", "worker"), None),
            P(("site", "handler", "worker")),
            P(("site", "handler", "worker"), None, None),
        ),
        out_specs=P(("site", "handler"), "worker", None, None),
        check_vma=False,
    )
```

```python
import functools

import jax
import jax.numpy as jnp
from jax import lax
from jax.experimental import pallas as pl
from jax.experimental.pallas import tpu as pltpu
from jax.sharding import PartitionSpec as P


TAPS = 64
BLK = 2
RUP_SLOTS = 4
LANES = 128
SUB = 8
PARTS = 2
VMEM_BUDGET = 12 * 1024 * 1024
MIB = 1024 * 1024
BF = jnp.bfloat16
F32 = jnp.float32


def combine_points(sgt, mechanism):
    total = mechanism[0].astype(jnp.float32)[:, None, None] * sgt[:, 0].astype(jnp.float32)
    for comp in range(1, 6):
        total = total + mechanism[comp].astype(jnp.float32)[:, None, None] * sgt[:, comp].astype(
            jnp.float32
        )
    return total.astype(jnp.bfloat16)


def shifted_blocks(green):
    samples = green.shape[-1]
    padded = jnp.pad(green, ((0, 0), (0, 0), (0, 0), (TAPS, 0)))
    return jnp.stack(
        [padded[..., TAPS - lag : TAPS - lag + samples] for lag in range(TAPS)], axis=2
    )


def deliver(first, second):
    return (
        lax.all_to_all(first, ("handler", "worker"), split_axis=0, concat_axis=0, tiled=True),
        lax.all_to_all(second, ("handler", "worker"), split_axis=0, concat_axis=0, tiled=True),
    )


def local_exchange(sgt, mechanism, req_owner, req_local, slip):
    peers = lax.axis_size(("handler", "worker"))
    samples = sgt.shape[-1]
    blocks_here = sgt.shape[0] // BLK
    requests = req_local.shape[0]
    capacity = max(2, (2 * requests + peers - 1) // peers)
    owner = req_owner[:, 0]
    member = (owner[:, None] == jnp.arange(peers, dtype=jnp.int32)[None, :]).astype(jnp.int32)
    earlier = jnp.sum((jnp.cumsum(member, axis=0) - member) * member, axis=1)
    position = owner * capacity + earlier
    table = jnp.full((peers * capacity,), -1, jnp.int32).at[position].set(req_local)
    asked = lax.all_to_all(
        table.reshape(peers, capacity),
        ("handler", "worker"),
        split_axis=0,
        concat_axis=0,
        tiled=True,
    )
    wanted = (asked >= 0).reshape(-1)
    picked = jnp.where(wanted, asked.reshape(-1), 0)
    green_here = combine_points(sgt, mechanism).reshape(blocks_here, BLK, 3, samples)
    chosen = jnp.where(wanted[:, None, None, None], green_here[picked], jnp.zeros((), jnp.bfloat16))
    chosen = chosen.reshape(peers, capacity, BLK, 3, samples)
    front, back = deliver(chosen[:, :, :, :2], chosen[:, :, :, 2:])
    arrived = jnp.concatenate([front, back], axis=3)
    blocks = arrived.reshape(peers * capacity, BLK, 3, samples)[position]
    rows = requests // RUP_SLOTS
    variations = slip.shape[1]
    outputs = []
    for slot in range(RUP_SLOTS):
        stacked = shifted_blocks(blocks[slot * rows : (slot + 1) * rows])
        right = stacked.reshape(rows * BLK * TAPS, 3 * samples)
        left = jnp.transpose(slip[slot * rows : (slot + 1) * rows], (1, 0, 2)).reshape(
            variations, rows * BLK * TAPS
        )
        outputs.append(
            jnp.dot(left, right, preferred_element_type=jnp.float32).reshape(variations, 3, samples)
        )
    partial_value = jnp.stack(outputs, axis=0)
    return lax.psum_scatter(partial_value, "worker", scatter_dimension=1, tiled=True)


def combine_kernel(samples, sgt_ref, mech_ref, same_ref, other_ref, mech_scratch):
    step = pl.program_id(0)
    count = same_ref.shape[0]

    @pl.when(step == 0)
    def _():
        mech_scratch[...] = jnp.transpose(mech_ref[...].astype(F32))

    mech = mech_scratch[pl.ds(pl.multiple_of(step * count, count), count), :]
    green = []
    for k in range(3):
        total = mech[:, 0:1] * sgt_ref[0, k].astype(F32)
        for comp in range(1, 6):
            total = total + mech[:, comp : comp + 1] * sgt_ref[comp, k].astype(F32)
        green.append(total.astype(BF))
    half = samples // 2
    parity = lax.rem(lax.axis_index("worker"), 2)

    def write(low_ref, high_ref):
        low_ref[:, :samples] = green[0]
        low_ref[:, samples : samples + LANES] = jnp.zeros((count, LANES), BF)
        low_ref[:, samples + LANES :] = green[1][:, :half]
        high_ref[:, :samples] = green[2]
        high_ref[:, samples:] = green[1][:, half - LANES :]

    @pl.when(parity == 0)
    def _():
        write(same_ref, other_ref)

    @pl.when(parity == 1)
    def _():
        write(other_ref, same_ref)


def combine(sgt, mechanism):
    points, comps, kinds, samples = sgt.shape
    width = samples + LANES + samples // 2
    step = min(16, points)
    out = jax.ShapeDtypeStruct((points, width), BF)
    return pl.pallas_call(
        functools.partial(combine_kernel, samples),
        grid=(points // step,),
        in_specs=[
            pl.BlockSpec((comps, kinds, step, samples), lambda p: (0, 0, p, 0)),
            pl.BlockSpec((comps, points), lambda p: (0, 0)),
        ],
        out_specs=[pl.BlockSpec((step, width), lambda p: (p, 0))] * 2,
        out_shape=[out, out],
        scratch_shapes=[pltpu.VMEM((points, comps), F32)],
        compiler_params=pltpu.CompilerParams(vmem_limit_bytes=16 * MIB),
        name="combine",
    )(jnp.transpose(sgt, (1, 2, 0, 3)), mechanism)


def group_transpose(rows, lane):
    rows = list(rows)
    count = len(rows)
    step = count // 2
    while step:
        keep = (lane // (SUB * step)) % 2 == 0
        for j in range(count):
            if j & step:
                continue
            low, high = rows[j], rows[j + step]
            rows[j] = jnp.where(keep, low, pltpu.roll(high, SUB * step, 1))
            rows[j + step] = jnp.where(keep, pltpu.roll(low, LANES - SUB * step, 1), high)
        step //= 2
    return rows


def turn_kernel(slip_ref, own_ref, *rest):
    others, grouped = rest[:-1], rest[-1]
    slots, coarse, group, _ = own_ref.shape
    rows = slip_ref.shape[0] // slots
    mine = lax.axis_index("worker") // 2
    tall = 2 * SUB
    lane = lax.broadcasted_iota(jnp.int32, (tall, LANES), 1)
    source = lax.broadcasted_iota(jnp.int32, (LANES, LANES), 0)
    target = lax.broadcasted_iota(jnp.int32, (LANES, LANES), 1)
    fine, row, point = source % SUB, (source % TAPS) // SUB, source // TAPS
    place = jnp.where(target == (fine * rows + row) * BLK + point, 1.0, 0.0).astype(BF)

    def turn(out, g, first, slot):
        for v in range(0, group, tall):
            at = pl.multiple_of((mine ^ g) * group + v, tall)
            turned = group_transpose(
                [slip_ref[(first + slot) * rows + n, pl.ds(at, tall), :] for n in range(rows)], lane
            )
            for a in range(coarse):
                grouped[a * group + v : a * group + v + tall, :] = turned[a]
        moved = jnp.dot(grouped[...], place, preferred_element_type=F32).astype(BF)
        for a in range(coarse):
            out[slot, a] = moved[a * group : (a + 1) * group]

    for index, out in enumerate(others):
        g, part = divmod(index, PARTS)
        first = part * out.shape[0]

        @pl.loop(0, out.shape[0])
        def _(slot, out=out, g=g, first=first):
            turn(out, g + 1, first, slot)

    @pl.loop(0, slots)
    def _(slot):
        turn(own_ref, 0, 0, slot)


def turn_slip(slip, workers):
    _, variations, depth = slip.shape
    groups = workers // 2
    group = variations // groups
    whole = jax.ShapeDtypeStruct((RUP_SLOTS, TAPS // SUB, group, depth), BF)
    piece = jax.ShapeDtypeStruct((RUP_SLOTS // PARTS, TAPS // SUB, group, depth), BF)
    outs = [whole] + [piece] * ((groups - 1) * PARTS)
    vmem = pl.BlockSpec(memory_space=pltpu.VMEM)
    return pl.pallas_call(
        turn_kernel,
        in_specs=[vmem],
        out_specs=[vmem] * len(outs),
        out_shape=outs,
        scratch_shapes=[pltpu.VMEM((TAPS // SUB * group, depth), BF)],
        compiler_params=pltpu.CompilerParams(vmem_limit_bytes=8 * MIB),
        name="turn_slip",
    )(slip)


def gather_kernel(rows_ref, *refs):
    green, dense, hot = refs[:-2], refs[-2], refs[-1]
    pieces = len(green)
    points, width = green[0].shape
    span = 2 * LANES
    asked = rows_ref[...]
    for c in range(0, pieces * points, LANES):
        column = lax.broadcasted_iota(jnp.int32, (asked.shape[0], LANES), 1) + c
        hot[:, c : c + LANES] = jnp.where(asked == column, 1.0, 0.0).astype(BF)
    together = max(1, span // points)
    for c in range(0, width, span):
        e = min(width, c + span)
        total = None
        for p in range(0, pieces, together):
            block = jnp.concatenate([g[:, c:e] for g in green[p : p + together]], axis=0)
            part = jnp.dot(
                hot[:, p * points : (p + together) * points], block, preferred_element_type=F32
            )
            total = part if total is None else total + part
        dense[:, c:e] = total.astype(BF)


def gather(rows, green):
    points, width = green[0].shape
    vmem = pl.BlockSpec(memory_space=pltpu.VMEM)
    return pl.pallas_call(
        gather_kernel,
        in_specs=[vmem] * (1 + len(green)),
        out_specs=vmem,
        out_shape=jax.ShapeDtypeStruct((rows.shape[0], width), BF),
        scratch_shapes=[pltpu.VMEM((rows.shape[0], len(green) * points), BF)],
        compiler_params=pltpu.CompilerParams(vmem_limit_bytes=8 * MIB),
        name="gather",
    )(rows, *green)


def convolve_kernel(base, dense, *refs):
    slips = refs[:-5]
    own_ref, send_ref, left, right, product = refs[-5:]
    sources = len(slips)
    width = dense.shape[1]
    slots = own_ref.shape[0]
    _, coarse, group, _ = slips[0].shape
    per_source = dense.shape[0] // (RUP_SLOTS * sources)
    tiles = width // LANES
    samples = (width - LANES) * 2 // 3
    first = samples // LANES
    parity = lax.rem(lax.axis_index("worker"), 2)
    span = 2 * LANES
    lane = lax.broadcasted_iota(jnp.int32, (SUB, LANES), 1)
    wide_lane = lax.broadcasted_iota(jnp.int32, (per_source, LANES), 1)
    zero = jnp.zeros((SUB, LANES), F32)

    def slot_body(slot, carry):
        for j in range(sources):
            for a in range(coarse):
                left[a * group : (a + 1) * group, j * LANES : (j + 1) * LANES] = slips[j][
                    slot + (base if slips[j].shape[0] > slots else 0), a
                ]
            at = pl.multiple_of(((base + slot) * sources + j) * per_source, per_source)
            for b in range(SUB):
                put = j * LANES + b * per_source
                before = jnp.zeros((per_source, LANES), BF)
                for m in range(tiles):
                    value = dense[pl.ds(at, per_source), m * LANES : (m + 1) * LANES]
                    if b:
                        turn = pltpu.roll(value, b, 1)
                        if m == first:
                            before = jnp.zeros((per_source, LANES), BF)
                        value = jnp.where(wide_lane < b, before, turn)
                        before = turn
                    right[put : put + per_source, m * LANES : (m + 1) * LANES] = value

        for c in range(0, width, span):
            e = min(width, c + span)
            product[:, c:e] = jnp.dot(left[...], right[:, c:e], preferred_element_type=F32)

        for side in range(2):
            for u in range(0, group // 2, SUB):
                total = [None] * tiles
                for a in range(coarse):
                    start = pl.multiple_of(
                        a * group + lax.rem(parity + side, 2) * (group // 2) + u, SUB
                    )
                    before = zero
                    for m in range(tiles):
                        value = product[pl.ds(start, SUB), m * LANES : (m + 1) * LANES]
                        if a:
                            value = pltpu.roll(value, a * SUB, 1)
                        if m == first:
                            before = zero
                        moved = jnp.where(lane < a * SUB, before, value) if a else value
                        before = value
                        total[m] = moved if total[m] is None else total[m] + moved
                total = total[:first] + total[first + 1 :]
                for m, value in enumerate(total):
                    if side == 0:
                        own_ref[slot, u : u + SUB, m * LANES : (m + 1) * LANES] = value
                    else:
                        send_ref[slot, u : u + SUB, m * LANES : (m + 1) * LANES] = value.astype(BF)
        return carry

    lax.fori_loop(0, slots, slot_body, 0)


def convolve(base, dense, slips):
    width = dense.shape[1]
    slots = slips[-1].shape[0]
    _, coarse, group, depth = slips[0].shape
    inner = depth * len(slips)
    vmem = pl.BlockSpec(memory_space=pltpu.VMEM)
    return pl.pallas_call(
        functools.partial(convolve_kernel, base),
        in_specs=[vmem] * (1 + len(slips)),
        out_specs=[vmem, vmem],
        out_shape=[
            jax.ShapeDtypeStruct((slots, group // 2, width - LANES), F32),
            jax.ShapeDtypeStruct((slots, group // 2, width - LANES), BF),
        ],
        scratch_shapes=[
            pltpu.VMEM((coarse * group, inner), BF),
            pltpu.VMEM((inner, width), BF),
            pltpu.VMEM((coarse * group, width), F32),
        ],
        compiler_params=pltpu.CompilerParams(vmem_limit_bytes=12 * MIB),
        name="convolve",
    )(dense, *slips)


def assemble_kernel(own_ref, got_ref, *refs):
    out_ref = refs[-1]
    _, _, _, samples = out_ref.shape
    half = samples // 2
    parity = lax.rem(lax.axis_index("worker"), 2)

    def write(low, high):
        out_ref[0, 0] = low[0, :, :samples].astype(F32)
        out_ref[0, 1, :, :half] = low[0, :, samples:].astype(F32)
        out_ref[0, 1, :, half:] = high[0, :, samples:].astype(F32)
        out_ref[0, 2] = high[0, :, :samples].astype(F32)

    @pl.when(parity == 0)
    def _():
        write(own_ref, got_ref)

    @pl.when(parity == 1)
    def _():
        write(got_ref, own_ref)


def assemble(base, own, got, samples, into):
    slots, group, width = own.shape
    spec = pl.BlockSpec((1, group, width), lambda r: (r, 0, 0))
    more = () if into is None else (into,)
    return pl.pallas_call(
        assemble_kernel,
        grid=(slots,),
        in_specs=[spec, spec] + [pl.BlockSpec(memory_space=pl.ANY)] * len(more),
        out_specs=pl.BlockSpec((1, 3, group, samples), lambda r: (base + r, 0, 0, 0)),
        out_shape=jax.ShapeDtypeStruct((RUP_SLOTS, 3, group, samples), F32),
        input_output_aliases={2: 0} if more else {},
        compiler_params=pltpu.CompilerParams(vmem_limit_bytes=8 * MIB),
        name="assemble",
    )(own, got, *more)


def swap(value, axis, flip):
    return lax.ppermute(value, axis, [(i, i ^ flip) for i in range(lax.axis_size(axis))])


def local_replicate(sgt, mechanism, req_owner, req_local, slip):
    handlers, workers = lax.axis_size("handler"), lax.axis_size("worker")
    handler, worker = lax.axis_index("handler"), lax.axis_index("worker")
    points, _, _, samples = sgt.shape
    blocks_here = points // BLK
    requests = req_local.shape[0]
    same, other = combine(sgt, mechanism)

    code = req_owner[:, 0] * blocks_here + req_local
    codes = jnp.stack([code] + [swap(code, "worker", flip) for flip in range(1, workers)])
    owner = codes // blocks_here
    piece = ((owner // workers) ^ handler) * workers + ((owner % workers) ^ worker)
    row = piece * points + codes % blocks_here * BLK
    row = jnp.transpose(row.reshape(workers, RUP_SLOTS, requests // RUP_SLOTS), (1, 0, 2))
    rows = (row[..., None] + jnp.arange(BLK, dtype=jnp.int32)).reshape(-1, 1)

    green = {(0, 0): same}
    for flip in range(1, workers):
        green[0, flip] = swap(other if flip % 2 else same, "worker", flip)
    green[0, workers - 1], rows = lax.optimization_barrier((green[0, workers - 1], rows))
    bit = handlers // 2
    while bit:
        for (hand, flip), value in list(green.items()):
            green[hand ^ bit, flip] = swap(value, "handler", bit)
        bit //= 2
    dense = gather(rows, [green[hand, flip] for hand in range(handlers) for flip in range(workers)])

    turned = turn_slip(slip, workers)
    near = [turned[0], swap(turned[0], "worker", 1)]
    out = None
    results = []
    for part in range(PARTS):
        slips = list(near)
        for flip in range(2, workers, 2):
            value = turned[1 + (flip // 2 - 1) * PARTS + part]
            slips.append(swap(value, "worker", flip))
            slips.append(swap(slips[-1], "worker", 1))
        own, send = convolve(part * RUP_SLOTS // PARTS, dense, slips)
        results.append((own, swap(send, "worker", 1)))
    for part, (own, got) in enumerate(results):
        out = assemble(part * RUP_SLOTS // PARTS, own, got, samples, out)
    return jnp.transpose(out, (0, 2, 1, 3))


def power_of_two(count):
    return count & (count - 1) == 0


def replicated(handlers, workers, points, kinds, samples, requests, variations, depth):
    width = samples + samples // 2 + LANES
    return (
        handlers * workers * points * width * 4 <= VMEM_BUDGET
        and power_of_two(handlers)
        and power_of_two(workers)
        and workers >= 2
        and kinds == 3
        and samples % (2 * LANES) == 0
        and depth == BLK * TAPS == LANES
        and requests // RUP_SLOTS == TAPS // SUB
        and variations % (workers * SUB) == 0
    )


def solution(mesh):
    handlers, workers = mesh.shape["handler"], mesh.shape["worker"]

    def local(sgt, mechanism, req_owner, req_local, slip):
        points, _, kinds, samples = sgt.shape
        requests, variations, depth = slip.shape
        if replicated(handlers, workers, points, kinds, samples, requests, variations, depth):
            return local_replicate(sgt, mechanism, req_owner, req_local, slip)
        return local_exchange(sgt, mechanism, req_owner, req_local, slip)

    return jax.shard_map(
        local,
        mesh=mesh,
        in_specs=(
            P(("site", "handler", "worker"), None, None, None),
            P(None, ("handler", "worker")),
            P(("site", "handler", "worker"), None),
            P(("site", "handler", "worker")),
            P(("site", "handler", "worker"), None, None),
        ),
        out_specs=P(("site", "handler"), "worker", None, None),
        check_vma=False,
    )
```

```python
import functools

import jax
import jax.numpy as jnp
from jax import lax
from jax.experimental import pallas as pl
from jax.experimental.pallas import tpu as pltpu
from jax.sharding import PartitionSpec as P


TAPS = 64
BLK = 2
RUP_SLOTS = 4
LANES = 128
SUB = 8
PARTS = 2
VMEM_BUDGET = 12 * 1024 * 1024
MIB = 1024 * 1024
BF = jnp.bfloat16
F32 = jnp.float32


def combine_points(sgt, mechanism):
    total = mechanism[0].astype(jnp.float32)[:, None, None] * sgt[:, 0].astype(jnp.float32)
    for comp in range(1, 6):
        total = total + mechanism[comp].astype(jnp.float32)[:, None, None] * sgt[:, comp].astype(
            jnp.float32
        )
    return total.astype(jnp.bfloat16)


def shifted_blocks(green):
    samples = green.shape[-1]
    padded = jnp.pad(green, ((0, 0), (0, 0), (0, 0), (TAPS, 0)))
    return jnp.stack(
        [padded[..., TAPS - lag : TAPS - lag + samples] for lag in range(TAPS)], axis=2
    )


def deliver(first, second):
    return (
        lax.all_to_all(first, ("handler", "worker"), split_axis=0, concat_axis=0, tiled=True),
        lax.all_to_all(second, ("handler", "worker"), split_axis=0, concat_axis=0, tiled=True),
    )


def local_exchange(sgt, mechanism, req_owner, req_local, slip):
    peers = lax.axis_size(("handler", "worker"))
    samples = sgt.shape[-1]
    blocks_here = sgt.shape[0] // BLK
    requests = req_local.shape[0]
    capacity = max(2, (2 * requests + peers - 1) // peers)
    owner = req_owner[:, 0]
    member = (owner[:, None] == jnp.arange(peers, dtype=jnp.int32)[None, :]).astype(jnp.int32)
    earlier = jnp.sum((jnp.cumsum(member, axis=0) - member) * member, axis=1)
    position = owner * capacity + earlier
    table = jnp.full((peers * capacity,), -1, jnp.int32).at[position].set(req_local)
    asked = lax.all_to_all(
        table.reshape(peers, capacity),
        ("handler", "worker"),
        split_axis=0,
        concat_axis=0,
        tiled=True,
    )
    wanted = (asked >= 0).reshape(-1)
    picked = jnp.where(wanted, asked.reshape(-1), 0)
    green_here = combine_points(sgt, mechanism).reshape(blocks_here, BLK, 3, samples)
    chosen = jnp.where(wanted[:, None, None, None], green_here[picked], jnp.zeros((), jnp.bfloat16))
    chosen = chosen.reshape(peers, capacity, BLK, 3, samples)
    front, back = deliver(chosen[:, :, :, :2], chosen[:, :, :, 2:])
    arrived = jnp.concatenate([front, back], axis=3)
    blocks = arrived.reshape(peers * capacity, BLK, 3, samples)[position]
    rows = requests // RUP_SLOTS
    variations = slip.shape[1]
    outputs = []
    for slot in range(RUP_SLOTS):
        stacked = shifted_blocks(blocks[slot * rows : (slot + 1) * rows])
        right = stacked.reshape(rows * BLK * TAPS, 3 * samples)
        left = jnp.transpose(slip[slot * rows : (slot + 1) * rows], (1, 0, 2)).reshape(
            variations, rows * BLK * TAPS
        )
        outputs.append(
            jnp.dot(left, right, preferred_element_type=jnp.float32).reshape(variations, 3, samples)
        )
    partial_value = jnp.stack(outputs, axis=0)
    return lax.psum_scatter(partial_value, "worker", scatter_dimension=1, tiled=True)


def combine_kernel(samples, sgt_ref, mech_ref, same_ref, other_ref, mech_scratch, sgt_scratch, sems):
    steps, comps, _, count, _ = sgt_scratch.shape

    def copy(step):
        rows = pl.ds(pl.multiple_of(step * count, count), count)
        return pltpu.make_async_copy(sgt_ref.at[:, :, rows, :], sgt_scratch.at[step], sems.at[step])

    for step in range(steps):
        copy(step).start()
    mech_scratch[...] = jnp.transpose(mech_ref[...].astype(F32))
    half = samples // 2
    parity = lax.rem(lax.axis_index("worker"), 2)

    @pl.loop(0, steps)
    def _(step):
        copy(step).wait()
        rows = pl.ds(pl.multiple_of(step * count, count), count)
        mech = mech_scratch[rows, :]
        green = []
        for k in range(3):
            total = mech[:, 0:1] * sgt_scratch[step, 0, k].astype(F32)
            for comp in range(1, comps):
                total = total + mech[:, comp : comp + 1] * sgt_scratch[step, comp, k].astype(F32)
            green.append(total.astype(BF))

        def write(low_ref, high_ref):
            low_ref[rows, :samples] = green[0]
            low_ref[rows, samples : samples + LANES] = jnp.zeros((count, LANES), BF)
            low_ref[rows, samples + LANES :] = green[1][:, :half]
            high_ref[rows, :samples] = green[2]
            high_ref[rows, samples:] = green[1][:, half - LANES :]

        @pl.when(parity == 0)
        def _():
            write(same_ref, other_ref)

        @pl.when(parity == 1)
        def _():
            write(other_ref, same_ref)


def combine(sgt, mechanism):
    points, comps, kinds, samples = sgt.shape
    width = samples + LANES + samples // 2
    count = min(16, points)
    steps = points // count
    out = jax.ShapeDtypeStruct((points, width), BF)
    vmem = pl.BlockSpec(memory_space=pltpu.VMEM)
    return pl.pallas_call(
        functools.partial(combine_kernel, samples),
        in_specs=[pl.BlockSpec(memory_space=pltpu.HBM), vmem],
        out_specs=[vmem] * 2,
        out_shape=[out, out],
        scratch_shapes=[
            pltpu.VMEM((points, comps), F32),
            pltpu.VMEM((steps, comps, kinds, count, samples), BF),
            pltpu.SemaphoreType.DMA((steps,)),
        ],
        compiler_params=pltpu.CompilerParams(vmem_limit_bytes=8 * MIB),
        name="combine",
    )(jnp.transpose(sgt, (1, 2, 0, 3)), mechanism)


def group_transpose(rows, lane):
    rows = list(rows)
    count = len(rows)
    step = count // 2
    while step:
        keep = (lane // (SUB * step)) % 2 == 0
        for j in range(count):
            if j & step:
                continue
            low, high = rows[j], rows[j + step]
            rows[j] = jnp.where(keep, low, pltpu.roll(high, SUB * step, 1))
            rows[j + step] = jnp.where(keep, pltpu.roll(low, LANES - SUB * step, 1), high)
        step //= 2
    return rows


def turn_kernel(slip_ref, own_ref, *rest):
    others, grouped = rest[:-1], rest[-1]
    slots, coarse, group, _ = own_ref.shape
    rows = slip_ref.shape[0] // slots
    mine = lax.axis_index("worker") // 2
    tall = 2 * SUB
    lane = lax.broadcasted_iota(jnp.int32, (tall, LANES), 1)
    source = lax.broadcasted_iota(jnp.int32, (LANES, LANES), 0)
    target = lax.broadcasted_iota(jnp.int32, (LANES, LANES), 1)
    fine, row, point = source % SUB, (source % TAPS) // SUB, source // TAPS
    place = jnp.where(target == (fine * rows + row) * BLK + point, 1.0, 0.0).astype(BF)

    def turn(out, g, first, slot):
        for v in range(0, group, tall):
            at = pl.multiple_of((mine ^ g) * group + v, tall)
            turned = group_transpose(
                [slip_ref[(first + slot) * rows + n, pl.ds(at, tall), :] for n in range(rows)], lane
            )
            for a in range(coarse):
                grouped[a * group + v : a * group + v + tall, :] = turned[a]
        moved = jnp.dot(grouped[...], place, preferred_element_type=F32).astype(BF)
        for a in range(coarse):
            out[slot, a] = moved[a * group : (a + 1) * group]

    for index, out in enumerate(others):
        g, part = divmod(index, PARTS)
        first = part * out.shape[0]

        @pl.loop(0, out.shape[0])
        def _(slot, out=out, g=g, first=first):
            turn(out, g + 1, first, slot)

    @pl.loop(0, slots)
    def _(slot):
        turn(own_ref, 0, 0, slot)


def turn_slip(slip, workers):
    _, variations, depth = slip.shape
    groups = workers // 2
    group = variations // groups
    whole = jax.ShapeDtypeStruct((RUP_SLOTS, TAPS // SUB, group, depth), BF)
    piece = jax.ShapeDtypeStruct((RUP_SLOTS // PARTS, TAPS // SUB, group, depth), BF)
    outs = [whole] + [piece] * ((groups - 1) * PARTS)
    vmem = pl.BlockSpec(memory_space=pltpu.VMEM)
    return pl.pallas_call(
        turn_kernel,
        in_specs=[vmem],
        out_specs=[vmem] * len(outs),
        out_shape=outs,
        scratch_shapes=[pltpu.VMEM((TAPS // SUB * group, depth), BF)],
        compiler_params=pltpu.CompilerParams(vmem_limit_bytes=8 * MIB),
        name="turn_slip",
    )(slip)


def gather_kernel(sources, *refs):
    codes, green, dense, hot = refs[:sources], refs[sources:-2], refs[-2], refs[-1]
    pieces = len(green)
    points, width = green[0].shape
    blocks_here = points // BLK
    requests = codes[0].shape[0] // RUP_SLOTS
    handler, worker = lax.axis_index("handler"), lax.axis_index("worker")
    tall = requests * BLK
    span = 2 * LANES
    row = lax.broadcasted_iota(jnp.int32, (tall, LANES), 0)
    lane = lax.broadcasted_iota(jnp.int32, (tall, LANES), 1)
    for slot in range(RUP_SLOTS):
        for j in range(sources):
            asked = jnp.zeros((tall, LANES), jnp.int32)
            for n in range(requests):
                code = codes[j][slot * requests + n]
                owner = code // blocks_here
                piece = ((owner // sources) ^ handler) * sources + (lax.rem(owner, sources) ^ worker)
                base = piece * points + lax.rem(code, blocks_here) * BLK - n * BLK
                asked = jnp.where(row >= n * BLK, base, asked)
            asked = asked + row - lane
            put = (slot * sources + j) * tall
            for c in range(0, pieces * points, LANES):
                hot[put : put + tall, c : c + LANES] = jnp.where(asked == c, 1.0, 0.0).astype(BF)
    together = max(1, span // points)
    for c in range(0, width, span):
        e = min(width, c + span)
        total = None
        for p in range(0, pieces, together):
            block = jnp.concatenate([g[:, c:e] for g in green[p : p + together]], axis=0)
            part = jnp.dot(
                hot[:, p * points : (p + together) * points], block, preferred_element_type=F32
            )
            total = part if total is None else total + part
        dense[:, c:e] = total.astype(BF)


def gather(codes, green):
    points, width = green[0].shape
    asked = len(codes) * codes[0].shape[0] * BLK
    vmem = pl.BlockSpec(memory_space=pltpu.VMEM)
    return pl.pallas_call(
        functools.partial(gather_kernel, len(codes)),
        in_specs=[pl.BlockSpec(memory_space=pltpu.SMEM)] * len(codes) + [vmem] * len(green),
        out_specs=vmem,
        out_shape=jax.ShapeDtypeStruct((asked, width), BF),
        scratch_shapes=[pltpu.VMEM((asked, len(green) * points), BF)],
        compiler_params=pltpu.CompilerParams(vmem_limit_bytes=8 * MIB),
        name="gather",
    )(*codes, *green)


def convolve_kernel(base, dense, *refs):
    slips = refs[:-5]
    own_ref, send_ref, left, right, product = refs[-5:]
    sources = len(slips)
    width = dense.shape[1]
    slots = own_ref.shape[0]
    _, coarse, group, _ = slips[0].shape
    per_source = dense.shape[0] // (RUP_SLOTS * sources)
    tiles = width // LANES
    samples = (width - LANES) * 2 // 3
    first = samples // LANES
    parity = lax.rem(lax.axis_index("worker"), 2)
    span = 2 * LANES
    lane = lax.broadcasted_iota(jnp.int32, (SUB, LANES), 1)
    wide_lane = lax.broadcasted_iota(jnp.int32, (per_source, LANES), 1)
    zero = jnp.zeros((SUB, LANES), F32)

    def slot_body(slot, carry):
        for j in range(sources):
            for a in range(coarse):
                left[a * group : (a + 1) * group, j * LANES : (j + 1) * LANES] = slips[j][
                    slot + (base if slips[j].shape[0] > slots else 0), a
                ]
            at = pl.multiple_of(((base + slot) * sources + j) * per_source, per_source)
            for b in range(SUB):
                put = j * LANES + b * per_source
                before = jnp.zeros((per_source, LANES), BF)
                for m in range(tiles):
                    value = dense[pl.ds(at, per_source), m * LANES : (m + 1) * LANES]
                    if b:
                        turn = pltpu.roll(value, b, 1)
                        if m == first:
                            before = jnp.zeros((per_source, LANES), BF)
                        value = jnp.where(wide_lane < b, before, turn)
                        before = turn
                    right[put : put + per_source, m * LANES : (m + 1) * LANES] = value

        for c in range(0, width, span):
            e = min(width, c + span)
            product[:, c:e] = jnp.dot(left[...], right[:, c:e], preferred_element_type=F32)

        for side in range(2):
            for u in range(0, group // 2, SUB):
                total = [None] * tiles
                for a in range(coarse):
                    start = pl.multiple_of(
                        a * group + lax.rem(parity + side, 2) * (group // 2) + u, SUB
                    )
                    before = zero
                    for m in range(tiles):
                        value = product[pl.ds(start, SUB), m * LANES : (m + 1) * LANES]
                        if a:
                            value = pltpu.roll(value, a * SUB, 1)
                        if m == first:
                            before = zero
                        moved = jnp.where(lane < a * SUB, before, value) if a else value
                        before = value
                        total[m] = moved if total[m] is None else total[m] + moved
                total = total[:first] + total[first + 1 :]
                for m, value in enumerate(total):
                    if side == 0:
                        own_ref[slot, u : u + SUB, m * LANES : (m + 1) * LANES] = value
                    else:
                        send_ref[slot, u : u + SUB, m * LANES : (m + 1) * LANES] = value.astype(BF)
        return carry

    lax.fori_loop(0, slots, slot_body, 0)


def convolve(base, dense, slips):
    width = dense.shape[1]
    slots = slips[-1].shape[0]
    _, coarse, group, depth = slips[0].shape
    inner = depth * len(slips)
    vmem = pl.BlockSpec(memory_space=pltpu.VMEM)
    return pl.pallas_call(
        functools.partial(convolve_kernel, base),
        in_specs=[vmem] * (1 + len(slips)),
        out_specs=[vmem, vmem],
        out_shape=[
            jax.ShapeDtypeStruct((slots, group // 2, width - LANES), F32),
            jax.ShapeDtypeStruct((slots, group // 2, width - LANES), BF),
        ],
        scratch_shapes=[
            pltpu.VMEM((coarse * group, inner), BF),
            pltpu.VMEM((inner, width), BF),
            pltpu.VMEM((coarse * group, width), F32),
        ],
        compiler_params=pltpu.CompilerParams(vmem_limit_bytes=12 * MIB),
        name="convolve",
    )(dense, *slips)


def assemble_kernel(own_ref, got_ref, *refs):
    out_ref = refs[-1]
    _, _, _, samples = out_ref.shape
    half = samples // 2
    parity = lax.rem(lax.axis_index("worker"), 2)

    def write(low, high):
        out_ref[0, 0] = low[0, :, :samples].astype(F32)
        out_ref[0, 1, :, :half] = low[0, :, samples:].astype(F32)
        out_ref[0, 1, :, half:] = high[0, :, samples:].astype(F32)
        out_ref[0, 2] = high[0, :, :samples].astype(F32)

    @pl.when(parity == 0)
    def _():
        write(own_ref, got_ref)

    @pl.when(parity == 1)
    def _():
        write(got_ref, own_ref)


def assemble(base, own, got, samples, into):
    slots, group, width = own.shape
    spec = pl.BlockSpec((1, group, width), lambda r: (r, 0, 0))
    more = () if into is None else (into,)
    return pl.pallas_call(
        assemble_kernel,
        grid=(slots,),
        in_specs=[spec, spec] + [pl.BlockSpec(memory_space=pl.ANY)] * len(more),
        out_specs=pl.BlockSpec((1, 3, group, samples), lambda r: (base + r, 0, 0, 0)),
        out_shape=jax.ShapeDtypeStruct((RUP_SLOTS, 3, group, samples), F32),
        input_output_aliases={2: 0} if more else {},
        compiler_params=pltpu.CompilerParams(vmem_limit_bytes=8 * MIB),
        name="assemble",
    )(own, got, *more)


def swap(value, axis, flip):
    return lax.ppermute(value, axis, [(i, i ^ flip) for i in range(lax.axis_size(axis))])


def local_replicate(sgt, mechanism, req_owner, req_local, slip):
    handlers, workers = lax.axis_size("handler"), lax.axis_size("worker")
    points, _, _, samples = sgt.shape
    same, other = combine(sgt, mechanism)

    code = req_owner[:, 0] * (points // BLK) + req_local
    codes = [code] + [swap(code, "worker", flip) for flip in range(1, workers)]

    green = {(0, 0): same}
    for flip in range(1, workers):
        green[0, flip] = swap(other if flip % 2 else same, "worker", flip)
    bit = handlers // 2
    while bit:
        for (hand, flip), value in list(green.items()):
            green[hand ^ bit, flip] = swap(value, "handler", bit)
        bit //= 2
    dense = gather(codes, [green[hand, flip] for hand in range(handlers) for flip in range(workers)])

    turned = turn_slip(slip, workers)
    near = [turned[0], swap(turned[0], "worker", 1)]
    out = None
    results = []
    for part in range(PARTS):
        slips = list(near)
        for flip in range(2, workers, 2):
            value = turned[1 + (flip // 2 - 1) * PARTS + part]
            slips.append(swap(value, "worker", flip))
            slips.append(swap(slips[-1], "worker", 1))
        own, send = convolve(part * RUP_SLOTS // PARTS, dense, slips)
        results.append((own, swap(send, "worker", 1)))
    for part, (own, got) in enumerate(results):
        out = assemble(part * RUP_SLOTS // PARTS, own, got, samples, out)
    return jnp.transpose(out, (0, 2, 1, 3))


def power_of_two(count):
    return count & (count - 1) == 0


def replicated(handlers, workers, points, kinds, samples, requests, variations, depth):
    width = samples + samples // 2 + LANES
    return (
        handlers * workers * points * width * 4 <= VMEM_BUDGET
        and power_of_two(handlers)
        and power_of_two(workers)
        and workers >= 2
        and kinds == 3
        and samples % (2 * LANES) == 0
        and depth == BLK * TAPS == LANES
        and requests // RUP_SLOTS == TAPS // SUB
        and variations % (workers * SUB) == 0
    )


def solution(mesh):
    handlers, workers = mesh.shape["handler"], mesh.shape["worker"]

    def local(sgt, mechanism, req_owner, req_local, slip):
        points, _, kinds, samples = sgt.shape
        requests, variations, depth = slip.shape
        if replicated(handlers, workers, points, kinds, samples, requests, variations, depth):
            return local_replicate(sgt, mechanism, req_owner, req_local, slip)
        return local_exchange(sgt, mechanism, req_owner, req_local, slip)

    return jax.shard_map(
        local,
        mesh=mesh,
        in_specs=(
            P(("site", "handler", "worker"), None, None, None),
            P(None, ("handler", "worker")),
            P(("site", "handler", "worker"), None),
            P(("site", "handler", "worker")),
            P(("site", "handler", "worker"), None, None),
        ),
        out_specs=P(("site", "handler"), "worker", None, None),
        check_vma=False,
    )
```

```python
import functools

import jax
import jax.numpy as jnp
from jax import lax
from jax.experimental import pallas as pl
from jax.experimental.pallas import tpu as pltpu
from jax.sharding import PartitionSpec as P


TAPS = 64
BLK = 2
RUP_SLOTS = 4
LANES = 128
SUB = 8
PARTS = 2
VMEM_BUDGET = 12 * 1024 * 1024
MIB = 1024 * 1024
BF = jnp.bfloat16
F32 = jnp.float32


def combine_points(sgt, mechanism):
    total = mechanism[0].astype(jnp.float32)[:, None, None] * sgt[:, 0].astype(jnp.float32)
    for comp in range(1, 6):
        total = total + mechanism[comp].astype(jnp.float32)[:, None, None] * sgt[:, comp].astype(
            jnp.float32
        )
    return total.astype(jnp.bfloat16)


def shifted_blocks(green):
    samples = green.shape[-1]
    padded = jnp.pad(green, ((0, 0), (0, 0), (0, 0), (TAPS, 0)))
    return jnp.stack(
        [padded[..., TAPS - lag : TAPS - lag + samples] for lag in range(TAPS)], axis=2
    )


def deliver(first, second):
    return (
        lax.all_to_all(first, ("handler", "worker"), split_axis=0, concat_axis=0, tiled=True),
        lax.all_to_all(second, ("handler", "worker"), split_axis=0, concat_axis=0, tiled=True),
    )


def local_exchange(sgt, mechanism, req_owner, req_local, slip):
    peers = lax.axis_size(("handler", "worker"))
    samples = sgt.shape[-1]
    blocks_here = sgt.shape[0] // BLK
    requests = req_local.shape[0]
    capacity = max(2, (2 * requests + peers - 1) // peers)
    owner = req_owner[:, 0]
    member = (owner[:, None] == jnp.arange(peers, dtype=jnp.int32)[None, :]).astype(jnp.int32)
    earlier = jnp.sum((jnp.cumsum(member, axis=0) - member) * member, axis=1)
    position = owner * capacity + earlier
    table = jnp.full((peers * capacity,), -1, jnp.int32).at[position].set(req_local)
    asked = lax.all_to_all(
        table.reshape(peers, capacity),
        ("handler", "worker"),
        split_axis=0,
        concat_axis=0,
        tiled=True,
    )
    wanted = (asked >= 0).reshape(-1)
    picked = jnp.where(wanted, asked.reshape(-1), 0)
    green_here = combine_points(sgt, mechanism).reshape(blocks_here, BLK, 3, samples)
    chosen = jnp.where(wanted[:, None, None, None], green_here[picked], jnp.zeros((), jnp.bfloat16))
    chosen = chosen.reshape(peers, capacity, BLK, 3, samples)
    front, back = deliver(chosen[:, :, :, :2], chosen[:, :, :, 2:])
    arrived = jnp.concatenate([front, back], axis=3)
    blocks = arrived.reshape(peers * capacity, BLK, 3, samples)[position]
    rows = requests // RUP_SLOTS
    variations = slip.shape[1]
    outputs = []
    for slot in range(RUP_SLOTS):
        stacked = shifted_blocks(blocks[slot * rows : (slot + 1) * rows])
        right = stacked.reshape(rows * BLK * TAPS, 3 * samples)
        left = jnp.transpose(slip[slot * rows : (slot + 1) * rows], (1, 0, 2)).reshape(
            variations, rows * BLK * TAPS
        )
        outputs.append(
            jnp.dot(left, right, preferred_element_type=jnp.float32).reshape(variations, 3, samples)
        )
    partial_value = jnp.stack(outputs, axis=0)
    return lax.psum_scatter(partial_value, "worker", scatter_dimension=1, tiled=True)


def combine_kernel(samples, sgt_ref, mech_ref, same_ref, other_ref, mech_scratch, sgt_scratch, sems):
    steps, comps, _, count, _ = sgt_scratch.shape

    def copy(step):
        rows = pl.ds(pl.multiple_of(step * count, count), count)
        return pltpu.make_async_copy(sgt_ref.at[:, :, rows, :], sgt_scratch.at[step], sems.at[step])

    for step in range(steps):
        copy(step).start()
    mech_scratch[...] = jnp.transpose(mech_ref[...])
    half = samples // 2
    parity = lax.rem(lax.axis_index("worker"), 2)

    @pl.loop(0, steps)
    def _(step):
        copy(step).wait()
        rows = pl.ds(pl.multiple_of(step * count, count), count)
        mech = mech_scratch[rows, :]
        green = []
        for k in range(3):
            total = mech[:, 0:1] * sgt_scratch[step, 0, k].astype(F32)
            for comp in range(1, comps):
                total = total + mech[:, comp : comp + 1] * sgt_scratch[step, comp, k].astype(F32)
            green.append(total.astype(BF))

        def write(low_ref, high_ref):
            low_ref[rows, :samples] = green[0]
            low_ref[rows, samples : samples + LANES] = jnp.zeros((count, LANES), BF)
            low_ref[rows, samples + LANES :] = green[1][:, :half]
            high_ref[rows, :samples] = green[2]
            high_ref[rows, samples:] = green[1][:, half - LANES :]

        @pl.when(parity == 0)
        def _():
            write(same_ref, other_ref)

        @pl.when(parity == 1)
        def _():
            write(other_ref, same_ref)


def combine(sgt, mechanism):
    points, comps, kinds, samples = sgt.shape
    width = samples + LANES + samples // 2
    count = min(16, points)
    steps = points // count
    out = jax.ShapeDtypeStruct((points, width), BF)
    vmem = pl.BlockSpec(memory_space=pltpu.VMEM)
    return pl.pallas_call(
        functools.partial(combine_kernel, samples),
        in_specs=[pl.BlockSpec(memory_space=pltpu.HBM), vmem],
        out_specs=[vmem] * 2,
        out_shape=[out, out],
        scratch_shapes=[
            pltpu.VMEM((points, comps), F32),
            pltpu.VMEM((steps, comps, kinds, count, samples), BF),
            pltpu.SemaphoreType.DMA((steps,)),
        ],
        compiler_params=pltpu.CompilerParams(vmem_limit_bytes=8 * MIB),
        name="combine",
    )(jnp.transpose(sgt, (1, 2, 0, 3)), mechanism.astype(F32))


def group_transpose(rows, lane):
    rows = list(rows)
    count = len(rows)
    step = count // 2
    while step:
        keep = (lane // (SUB * step)) % 2 == 0
        for j in range(count):
            if j & step:
                continue
            low, high = rows[j], rows[j + step]
            rows[j] = jnp.where(keep, low, pltpu.roll(high, SUB * step, 1))
            rows[j + step] = jnp.where(keep, pltpu.roll(low, LANES - SUB * step, 1), high)
        step //= 2
    return rows


def turn_kernel(slip_ref, own_ref, *rest):
    others, grouped = rest[:-1], rest[-1]
    slots, coarse, group, _ = own_ref.shape
    rows = slip_ref.shape[0] // slots
    mine = lax.axis_index("worker") // 2
    tall = 2 * SUB
    lane = lax.broadcasted_iota(jnp.int32, (tall, LANES), 1)
    source = lax.broadcasted_iota(jnp.int32, (LANES, LANES), 0)
    target = lax.broadcasted_iota(jnp.int32, (LANES, LANES), 1)
    fine, row, point = source % SUB, (source % TAPS) // SUB, source // TAPS
    place = jnp.where(target == (fine * rows + row) * BLK + point, 1.0, 0.0).astype(BF)

    def turn(out, g, first, slot):
        for v in range(0, group, tall):
            at = pl.multiple_of((mine ^ g) * group + v, tall)
            turned = group_transpose(
                [slip_ref[(first + slot) * rows + n, pl.ds(at, tall), :] for n in range(rows)], lane
            )
            for a in range(coarse):
                grouped[a * group + v : a * group + v + tall, :] = turned[a]
        moved = jnp.dot(grouped[...], place, preferred_element_type=F32).astype(BF)
        for a in range(coarse):
            out[slot, a] = moved[a * group : (a + 1) * group]

    for index, out in enumerate(others):
        g, part = divmod(index, PARTS)
        first = part * out.shape[0]

        @pl.loop(0, out.shape[0])
        def _(slot, out=out, g=g, first=first):
            turn(out, g + 1, first, slot)

    @pl.loop(0, slots)
    def _(slot):
        turn(own_ref, 0, 0, slot)


def turn_slip(slip, workers):
    _, variations, depth = slip.shape
    groups = workers // 2
    group = variations // groups
    whole = jax.ShapeDtypeStruct((RUP_SLOTS, TAPS // SUB, group, depth), BF)
    piece = jax.ShapeDtypeStruct((RUP_SLOTS // PARTS, TAPS // SUB, group, depth), BF)
    outs = [whole] + [piece] * ((groups - 1) * PARTS)
    vmem = pl.BlockSpec(memory_space=pltpu.VMEM)
    return pl.pallas_call(
        turn_kernel,
        in_specs=[vmem],
        out_specs=[vmem] * len(outs),
        out_shape=outs,
        scratch_shapes=[pltpu.VMEM((TAPS // SUB * group, depth), BF)],
        compiler_params=pltpu.CompilerParams(vmem_limit_bytes=8 * MIB),
        name="turn_slip",
    )(slip)


def hot_rows(hot, codes, slots, picks, points, here):
    requests = codes[0].shape[0] // RUP_SLOTS
    tall = requests * BLK
    row = lax.broadcasted_iota(jnp.int32, (tall, LANES), 0)
    lane = lax.broadcasted_iota(jnp.int32, (tall, LANES), 1)
    per = LANES // points
    columns = []
    for p in range(0, len(picks), per):
        column = lane + (picks[p] * points)
        for q in range(1, per):
            column = jnp.where(lane >= q * points, lane + (picks[p + q] - q) * points, column)
        columns.append(column - row)
    for index, slot in enumerate(slots):
        for j, code in enumerate(codes):
            asked = None
            for n in range(requests):
                base = (code[slot * requests + n] ^ here) - n * BLK
                asked = jnp.full((tall, LANES), base) if n == 0 else jnp.where(row >= n * BLK, base, asked)
            put = (index * len(codes) + j) * tall
            for c, column in enumerate(columns):
                hot[put : put + tall, c * LANES : (c + 1) * LANES] = jnp.where(
                    asked == column, 1.0, 0.0
                ).astype(BF)


def picked(hot, green, lo, hi):
    points = green[0].shape[0]
    together = max(1, 2 * LANES // points)
    total = None
    for p in range(0, len(green), together):
        block = jnp.concatenate([g[:, lo:hi] for g in green[p : p + together]], axis=0)
        part = jnp.dot(
            hot[:, p * points : (p + together) * points], block, preferred_element_type=F32
        )
        total = part if total is None else total + part
    return total


def my_place(workers, points):
    return (lax.axis_index("handler") * workers + lax.axis_index("worker")) * points


def gather_kernel(sources, picks, *refs):
    codes, green, dense, hot = refs[:sources], refs[sources:-2], refs[-2], refs[-1]
    points, width = green[0].shape
    hot_rows(hot, codes, range(RUP_SLOTS), picks, points, my_place(sources, points))
    for c in range(0, width, 2 * LANES):
        e = min(width, c + 2 * LANES)
        dense[:, c:e] = picked(hot, green, c, e).astype(BF)


def gather(codes, picks, green):
    points, width = green[0].shape
    asked = len(codes) * codes[0].shape[0] * BLK
    vmem = pl.BlockSpec(memory_space=pltpu.VMEM)
    return pl.pallas_call(
        functools.partial(gather_kernel, len(codes), picks),
        in_specs=[pl.BlockSpec(memory_space=pltpu.SMEM)] * len(codes) + [vmem] * len(green),
        out_specs=vmem,
        out_shape=jax.ShapeDtypeStruct((asked, width), BF),
        scratch_shapes=[pltpu.VMEM((asked, len(green) * points), BF)],
        compiler_params=pltpu.CompilerParams(vmem_limit_bytes=8 * MIB),
        name="gather",
    )(*codes, *green)


def convolve_kernel(base, picks, sources, *refs):
    codes, given, refs = refs[:sources], refs[sources], refs[sources + 1 :]
    green, refs = refs[: len(picks)], refs[len(picks) :]
    slips, refs = refs[:sources], refs[sources:]
    own_ref, send_ref, hot, dense, left, right, product = refs
    points, width = green[0].shape
    slots = own_ref.shape[0]
    _, coarse, group, _ = slips[0].shape
    asked = given.shape[0] // RUP_SLOTS
    per_source = asked // sources
    tiles = width // LANES
    samples = (width - LANES) * 2 // 3
    first = samples // LANES
    parity = lax.rem(lax.axis_index("worker"), 2)
    span = 2 * LANES

    hot_rows(hot, codes, range(base, base + slots), picks, points, my_place(sources, points))
    for c in range(0, width, span):
        e = min(width, c + span)
        had = given[base * asked : (base + slots) * asked, c:e].astype(F32)
        dense[:, c:e] = (had + picked(hot, green, c, e)).astype(BF)

    lane = lax.broadcasted_iota(jnp.int32, (SUB, LANES), 1)
    wide_lane = lax.broadcasted_iota(jnp.int32, (per_source, LANES), 1)
    zero = jnp.zeros((SUB, LANES), F32)

    for slot in range(slots):
        for j in range(sources):
            for a in range(coarse):
                left[slot, a * group : (a + 1) * group, j * LANES : (j + 1) * LANES] = slips[j][
                    slot + (base if slips[j].shape[0] > slots else 0), a
                ]
            at = (slot * sources + j) * per_source
            for b in range(SUB):
                put = j * LANES + b * per_source
                before = jnp.zeros((per_source, LANES), BF)
                for m in range(tiles):
                    value = dense[at : at + per_source, m * LANES : (m + 1) * LANES]
                    if b:
                        turn = pltpu.roll(value, b, 1)
                        if m == first:
                            before = jnp.zeros((per_source, LANES), BF)
                        value = jnp.where(wide_lane < b, before, turn)
                        before = turn
                    right[slot, put : put + per_source, m * LANES : (m + 1) * LANES] = value

        for c in range(0, width, span):
            e = min(width, c + span)
            product[slot, :, c:e] = jnp.dot(
                left[slot], right[slot, :, c:e], preferred_element_type=F32
            )

        for side in range(2):
            for u in range(0, group // 2, SUB):
                total = [None] * tiles
                for a in range(coarse):
                    start = pl.multiple_of(
                        a * group + lax.rem(parity + side, 2) * (group // 2) + u, SUB
                    )
                    before = zero
                    for m in range(tiles):
                        value = product[slot, pl.ds(start, SUB), m * LANES : (m + 1) * LANES]
                        if a:
                            value = pltpu.roll(value, a * SUB, 1)
                        if m == first:
                            before = zero
                        moved = jnp.where(lane < a * SUB, before, value) if a else value
                        before = value
                        total[m] = moved if total[m] is None else total[m] + moved
                total = total[:first] + total[first + 1 :]
                for m, value in enumerate(total):
                    if side == 0:
                        own_ref[slot, u : u + SUB, m * LANES : (m + 1) * LANES] = value
                    else:
                        send_ref[slot, u : u + SUB, m * LANES : (m + 1) * LANES] = value.astype(BF)


def convolve(base, codes, given, picks, green, slips):
    points, width = green[0].shape
    slots = slips[-1].shape[0]
    _, coarse, group, depth = slips[0].shape
    inner = depth * len(slips)
    asked = given.shape[0] // RUP_SLOTS * slots
    vmem = pl.BlockSpec(memory_space=pltpu.VMEM)
    smem = pl.BlockSpec(memory_space=pltpu.SMEM)
    return pl.pallas_call(
        functools.partial(convolve_kernel, base, picks, len(slips)),
        in_specs=[smem] * len(codes) + [vmem] * (1 + len(green) + len(slips)),
        out_specs=[vmem, vmem],
        out_shape=[
            jax.ShapeDtypeStruct((slots, group // 2, width - LANES), F32),
            jax.ShapeDtypeStruct((slots, group // 2, width - LANES), BF),
        ],
        scratch_shapes=[
            pltpu.VMEM((asked, len(green) * points), BF),
            pltpu.VMEM((asked, width), BF),
            pltpu.VMEM((slots, coarse * group, inner), BF),
            pltpu.VMEM((slots, inner, width), BF),
            pltpu.VMEM((slots, coarse * group, width), F32),
        ],
        compiler_params=pltpu.CompilerParams(vmem_limit_bytes=16 * MIB),
        name="convolve",
    )(*codes, given, *green, *slips)


def assemble_kernel(own_ref, got_ref, *refs):
    out_ref = refs[-1]
    _, _, _, samples = out_ref.shape
    half = samples // 2
    parity = lax.rem(lax.axis_index("worker"), 2)

    def write(low, high):
        out_ref[0, 0] = low[0, :, :samples].astype(F32)
        out_ref[0, 1, :, :half] = low[0, :, samples:].astype(F32)
        out_ref[0, 1, :, half:] = high[0, :, samples:].astype(F32)
        out_ref[0, 2] = high[0, :, :samples].astype(F32)

    @pl.when(parity == 0)
    def _():
        write(own_ref, got_ref)

    @pl.when(parity == 1)
    def _():
        write(got_ref, own_ref)


def assemble(base, own, got, samples, into):
    slots, group, width = own.shape
    spec = pl.BlockSpec((1, group, width), lambda r: (r, 0, 0))
    more = () if into is None else (into,)
    return pl.pallas_call(
        assemble_kernel,
        grid=(slots,),
        in_specs=[spec, spec] + [pl.BlockSpec(memory_space=pl.ANY)] * len(more),
        out_specs=pl.BlockSpec((1, 3, group, samples), lambda r: (base + r, 0, 0, 0)),
        out_shape=jax.ShapeDtypeStruct((RUP_SLOTS, 3, group, samples), F32),
        input_output_aliases={2: 0} if more else {},
        compiler_params=pltpu.CompilerParams(vmem_limit_bytes=8 * MIB),
        name="assemble",
    )(own, got, *more)


def swap(value, axis, flip):
    return lax.ppermute(value, axis, [(i, i ^ flip) for i in range(lax.axis_size(axis))])


def local_replicate(sgt, mechanism, req_owner, req_local, slip):
    handlers, workers = lax.axis_size("handler"), lax.axis_size("worker")
    points, _, _, samples = sgt.shape
    same, other = combine(sgt, mechanism)

    code = req_owner[:, 0] * points + req_local * BLK
    codes = [code] + [swap(code, "worker", flip) for flip in range(1, workers)]

    green = {(0, 0): same}
    for flip in range(1, workers):
        green[0, flip] = swap(other if flip % 2 else same, "worker", flip)
    bit = handlers // 2
    while bit:
        for (hand, flip), value in list(green.items()):
            green[hand ^ bit, flip] = swap(value, "handler", bit)
        bit //= 2
    last = [hand * workers + workers - 1 for hand in range(handlers)]
    early = [pick for pick in range(handlers * workers) if pick not in last]
    piece = [green[divmod(pick, workers)] for pick in range(handlers * workers)]
    given = gather(codes, early, [piece[pick] for pick in early])

    turned = turn_slip(slip, workers)
    near = [turned[0], swap(turned[0], "worker", 1)]
    out = None
    results = []
    for part in range(PARTS):
        slips = list(near)
        for flip in range(2, workers, 2):
            value = turned[1 + (flip // 2 - 1) * PARTS + part]
            slips.append(swap(value, "worker", flip))
            slips.append(swap(slips[-1], "worker", 1))
        own, send = convolve(
            part * RUP_SLOTS // PARTS, codes, given, last, [piece[pick] for pick in last], slips
        )
        results.append((own, swap(send, "worker", 1)))
    for part, (own, got) in enumerate(results):
        out = assemble(part * RUP_SLOTS // PARTS, own, got, samples, out)
    return jnp.transpose(out, (0, 2, 1, 3))


def power_of_two(count):
    return count & (count - 1) == 0


def replicated(handlers, workers, points, kinds, samples, requests, variations, depth):
    width = samples + samples // 2 + LANES
    return (
        handlers * workers * points * width * 4 <= VMEM_BUDGET
        and power_of_two(handlers)
        and power_of_two(workers)
        and power_of_two(points)
        and points <= LANES
        and workers >= 2
        and handlers * points % LANES == 0
        and kinds == 3
        and samples % (2 * LANES) == 0
        and depth == BLK * TAPS == LANES
        and requests // RUP_SLOTS == TAPS // SUB
        and variations % (workers * SUB) == 0
    )


def solution(mesh):
    handlers, workers = mesh.shape["handler"], mesh.shape["worker"]

    def local(sgt, mechanism, req_owner, req_local, slip):
        points, _, kinds, samples = sgt.shape
        requests, variations, depth = slip.shape
        if replicated(handlers, workers, points, kinds, samples, requests, variations, depth):
            return local_replicate(sgt, mechanism, req_owner, req_local, slip)
        return local_exchange(sgt, mechanism, req_owner, req_local, slip)

    return jax.shard_map(
        local,
        mesh=mesh,
        in_specs=(
            P(("site", "handler", "worker"), None, None, None),
            P(None, ("handler", "worker")),
            P(("site", "handler", "worker"), None),
            P(("site", "handler", "worker")),
            P(("site", "handler", "worker"), None, None),
        ),
        out_specs=P(("site", "handler"), "worker", None, None),
        check_vma=False,
    )
```
